32 devices in a mesh: dp: 16 (over z, x, core), emb: 2 (over y).
Axes of the slice: x: 2, y: 2, z: 4, core: 2. Of those that a mesh axis runs over, the one named last changes fastest.
Arguments:
- cur_ids: int32 [8192], P(('dp', 'emb')), may hold values from 0 to 3071, as said below
- prev_ids: int32 [8192], P(('dp', 'emb')), may hold values from 0 to 3071, as said below
- prev_grads: bfloat16 [8192, 128], P(('dp', 'emb')), may hold values from -6 to 6
- row_place: int32 [3072], replicated, may hold values from 0 to 3071, as said below
- table: float32 [3072, 128], P('emb'), may hold values from -6 to 6
- accum: float32 [3072, 128], P('emb'), may hold values from 0.05 to 2
- labels: float32 [8192], P('dp'), may hold values from 0 to 1
- gain: float32 [128], replicated, may hold values from 0.5 to 1.5
- w_gate: bfloat16 [128, 4096], P(None, 'emb'), may hold values from -0.5 to 0.5
- w_up: bfloat16 [128, 4096], P(None, 'emb'), may hold values from -0.5 to 0.5
- w_out: bfloat16 [4096], P('emb'), may hold values from -0.09375 to 0.09375
Outputs:
- new_table: float32 [3072, 128], P('emb')
- new_accum: float32 [3072, 128], P('emb')
- grad_gate: float32 [128, 4096], P(None, 'emb')
- grad_up: float32 [128, 4096], P(None, 'emb')
- emb_grad: float32 [8192, 128], P(('dp', 'emb'))
The draws below stay inside these ranges and needn't reach their ends.
Inputs may be any that keep to these rules, and one draw needn't show every extreme that they name: A permutation of the table rows; row i is stored on shard row_place[i] // 1536 of emb at position row_place[i] % 1536. `cur_ids`: the 256 ids of one device name rows of one shard at most 256 times, and exactly 256 times for some shard. `prev_ids`: the 256 ids of one device name rows of one shard at most 256 times, and exactly 256 times for some shard.
All inputs are finite; a program needn't handle non-finite values.
Results may differ from the reference program's by a relative error of at most 0.0069.
Values may be sent and summed in bfloat16 or wider, within the bound.
A program may use at most 64 MiB of HBM per device.

```python
import math
import jax
import jax.numpy as jnp
from jax import lax

E = 128
HID = 4096
TOK_DEV = 256
ROWS_SHARD = 1536
TOKENS = 8192
VOCAB = 3072
CAP = 256
N_DP = 16
N_EMB = 2


def place_table(key):
    return jax.random.permutation(jax.random.fold_in(key, 11), VOCAB).astype(jnp.int32)


def draw_ids(key, salt):
    placement = place_table(key)
    inverse = jnp.zeros((VOCAB,), jnp.int32).at[placement].set(jnp.arange(VOCAB, dtype=jnp.int32))
    blocks = TOKENS // TOK_DEV
    salted = jax.random.fold_in(key, salt)
    hot_shard = jax.random.randint(jax.random.fold_in(salted, 1), (blocks, 1), 0, N_EMB)
    position = jnp.arange(TOK_DEV, dtype=jnp.int32)[None, :]
    others = (hot_shard + 1 + (position - CAP) % max(N_EMB - 1, 1)) % N_EMB
    target = jnp.where(position < CAP, hot_shard, others)
    device_keys = jax.random.split(jax.random.fold_in(salted, 2), blocks)
    shuffle = jax.vmap(lambda one_key: jax.random.permutation(one_key, TOK_DEV))(device_keys)
    target = jnp.take_along_axis(target, shuffle, axis=1)
    first_pick = jax.random.randint(jax.random.fold_in(salted, 3), (blocks, TOK_DEV), 0, ROWS_SHARD)
    second_pick = jax.random.randint(jax.random.fold_in(salted, 4), (blocks, TOK_DEV), 0, ROWS_SHARD)
    slot_index = jnp.minimum(first_pick, second_pick)
    return inverse[target * ROWS_SHARD + slot_index].reshape(TOKENS).astype(jnp.int32)


def draw_row_place(key, part):
    return place_table(key)


def draw_cur_ids(key, part):
    return draw_ids(key, 21)


def draw_prev_ids(key, part):
    return draw_ids(key, 22)


def level_of(key, shape, cuts, smallest, top_value):
    def one(dim, blocks):
        steps = jax.random.uniform(jax.random.fold_in(jax.random.fold_in(key, 6), dim), (blocks,), jnp.float32, smallest / len(cuts), top_value / len(cuts))
        return jnp.repeat(jnp.exp(steps), shape[dim] // blocks).reshape((-1,) + (1,) * (len(shape) - dim - 1))

    factor_of = one(*cuts[0])
    for cut in cuts[1:]:
        factor_of = factor_of * one(*cut)
    return factor_of


def normal_values(rng, dims, deviation, reach, pieces=(), held_as=jnp.bfloat16):
    entries = deviation * jax.random.normal(rng, dims, jnp.float32)
    if pieces:
        entries = entries * level_of(rng, dims, pieces, -0.22, 0.18)
    return jnp.clip(entries, -reach, reach).astype(held_as)


def setup_inputs(seed: int = 0) -> dict:
    key_of = jax.random.split(jax.random.key(seed), 12)
    cur_ids = draw_cur_ids(jax.random.fold_in(key_of[11], 71), 0)
    prev_ids = draw_prev_ids(jax.random.fold_in(key_of[11], 71), 0)
    prev_grads = normal_values(key_of[2], (TOKENS, E), 1.0, 6.0, ((0, 32),))
    row_place = draw_row_place(jax.random.fold_in(key_of[11], 71), 0)
    table = normal_values(key_of[4], (VOCAB, E), 1.0, 6.0, ((0, 2),), jnp.float32)
    accum = jnp.clip(jnp.exp(math.log(2.0) - 3.6888794 * jax.random.uniform(key_of[5], (VOCAB, E), jnp.float32) ** level_of(key_of[5], (VOCAB, E), ((0, 2),), -0.2, 0.2)), 0.05, 2.0)
    labels = jnp.clip(1.0 * jax.random.uniform(key_of[6], (TOKENS,), jnp.float32) ** level_of(key_of[6], (TOKENS,), ((0, 16),), -0.2, 0.2), 0.0, 1.0)
    gain = jnp.clip(1.0 + 0.1 * jax.random.normal(key_of[7], (E,), jnp.float32), 0.5, 1.5)
    w_gate = normal_values(key_of[8], (E, HID), E ** -0.5, 0.5, ((1, 2),))
    w_up = normal_values(key_of[9], (E, HID), E ** -0.5, 0.5, ((1, 2),))
    w_out = normal_values(key_of[10], (HID,), HID ** -0.5, 0.09375, ((0, 2),))
    return {"cur_ids": cur_ids, "prev_ids": prev_ids, "prev_grads": prev_grads, "row_place": row_place, "table": table, "accum": accum, "labels": labels, "gain": gain, "w_gate": w_gate, "w_up": w_up, "w_out": w_out}


loss_weight = 64.0
learn_rate = 0.1
norm_eps = 1e-06

def reference(cur_ids, prev_ids, prev_grads, row_place, table, accum, labels, gain, w_gate, w_up, w_out):
    gain_f = gain.astype(jnp.float32)

    def tower_block(sums_so_far, blocked):
        positions, targets = blocked
        looked_up = table[positions].astype(jnp.bfloat16)
        values = looked_up.astype(jnp.float32)
        inverse_rms = lax.rsqrt(lax.optimization_barrier(jnp.mean(values * values, axis=1, keepdims=True)) + norm_eps)
        normed = (values * inverse_rms * gain_f).astype(jnp.bfloat16)
        gate_proj = jnp.dot(normed, w_gate, preferred_element_type=jnp.float32)
        up_proj = jnp.dot(normed, w_up, preferred_element_type=jnp.float32)
        sigmoid_gate = jax.nn.sigmoid(gate_proj)
        activated = gate_proj * sigmoid_gate
        hidden = (activated * up_proj).astype(jnp.bfloat16)
        logits = jnp.dot(hidden, w_out, preferred_element_type=jnp.float32)
        slopes = loss_weight * (jax.nn.sigmoid(logits) - targets)
        back_hidden = slopes[:, None] * w_out.astype(jnp.float32)[None, :]
        back_gate = (back_hidden * up_proj * sigmoid_gate * (1.0 + gate_proj * (1.0 - sigmoid_gate))).astype(jnp.bfloat16)
        back_up = (back_hidden * activated).astype(jnp.bfloat16)
        contract = (((0,), (0,)), ((), ()))
        gate_part = lax.dot_general(normed, back_gate, contract, preferred_element_type=jnp.float32)
        up_part = lax.dot_general(normed, back_up, contract, preferred_element_type=jnp.float32)
        across = (((1,), (1,)), ((), ()))
        back_normed = lax.dot_general(back_gate, w_gate, across, preferred_element_type=jnp.float32)
        back_normed = back_normed + lax.dot_general(back_up, w_up, across, preferred_element_type=jnp.float32)
        scaled = back_normed * gain_f
        row_grad = inverse_rms * scaled - values * inverse_rms ** 3 * lax.optimization_barrier(jnp.mean(values * scaled, axis=1, keepdims=True))
        return ((sums_so_far[0] + gate_part, sums_so_far[1] + up_part), row_grad)
    positions = row_place[cur_ids].reshape(N_DP, -1)
    targets = labels.reshape(N_DP, -1)
    start_sums = (jnp.zeros((E, HID), jnp.float32), jnp.zeros((E, HID), jnp.float32))
    (gate_sum, up_sum), row_grads = lax.scan(tower_block, start_sums, (positions, targets))
    tower_scale = 1.0 / math.sqrt(TOKENS)
    table_grad = jax.ops.segment_sum(prev_grads.astype(jnp.float32), row_place[prev_ids], num_segments=VOCAB)
    new_accum = accum + table_grad * table_grad
    new_table = table - learn_rate * table_grad * lax.rsqrt(new_accum)
    return (new_table, new_accum, gate_sum * tower_scale, up_sum * tower_scale, row_grads.reshape(TOKENS, E))
```

```python
import functools
import math

import jax
import jax.numpy as jnp
from jax import lax
from jax.experimental import pallas as pl
from jax.experimental.pallas import tpu as pltpu
from jax.sharding import PartitionSpec as P

loss_weight = 64.0
learn_rate = 0.1
norm_eps = 1e-06
MESH = pl.DeviceIdType.MESH
F32 = jnp.float32
BF16 = jnp.bfloat16


def dot(a, b):
    return jnp.dot(a, b, preferred_element_type=F32)


def dot_nt(a, b):
    return lax.dot_general(a, b, (((1,), (1,)), ((), ())), preferred_element_type=F32)


def tower_kernel(
    n_dp,
    n_emb,
    scale,
    cur_ref,
    prev_ref,
    grads_ref,
    place_ref,
    table_ref,
    labels_ref,
    gain_ref,
    wg_ref,
    wu_ref,
    wo_ref,
    total_ref,
    gate_ref,
    up_ref,
    emb_ref,
    table16,
    posall,
    gall,
    contrib,
    lbuf,
    values,
    normed,
    normed_t,
    act,
    logit,
    logit_in,
    slopes,
    bn,
    bn_in,
    tpart,
    tpair,
    tsum,
    tin,
    tall,
    gpart,
    gpair,
    gsum,
    gin,
    gall_sum,
    e_send,
    e_recv,
    t_send,
    t_recv,
    g_send,
    g_recv,
):
    me_dp = lax.axis_index("dp")
    me_emb = lax.axis_index("emb")
    n_chip = n_dp // 2
    chip = me_dp // 2
    par = me_dp % 2
    other = 1 - par
    partner = me_dp + 1 - 2 * par
    tok = grads_ref.shape[0]
    rows = table_ref.shape[0]
    hid = wg_ref.shape[1]
    ht = 256
    t_rows = rows // n_dp
    g_rows = hid // n_chip

    def copy(src, dst, send, recv, dp, emb):
        return pltpu.make_async_remote_copy(
            src_ref=src,
            dst_ref=dst,
            send_sem=send,
            recv_sem=recv,
            device_id=(dp, emb),
            device_id_type=MESH,
        )

    emb_peers = [lax.rem(me_emb + k, n_emb) for k in range(1, n_emb)]
    chip_peers = [2 * lax.rem(chip + k, n_chip) + par for k in range(1, n_chip)]
    from_chip = [lax.rem(chip + n_chip - k, n_chip) for k in range(1, n_chip)]

    barrier = pltpu.get_barrier_semaphore()
    for peer in emb_peers:
        pl.semaphore_signal(barrier, inc=1, device_id=(me_dp, peer), device_id_type=MESH)
    for peer in chip_peers:
        pl.semaphore_signal(barrier, inc=1, device_id=(peer, me_emb), device_id_type=MESH)
    pl.semaphore_signal(barrier, inc=1, device_id=(partner, me_emb), device_id_type=MESH)

    ids = jnp.concatenate([cur_ref[...], prev_ref[...]], axis=1)
    step = 512

    def place_step(i, acc):
        at = pl.multiple_of(i * step, step)
        part = place_ref[:, pl.ds(at, step)]
        both = jnp.broadcast_to(part, (8, step))
        lane_row = lax.broadcasted_iota(jnp.int32, (8, step), 0)
        halves = jnp.where(lane_row == 0, both >> 6, both & 63).astype(F32).astype(BF16)
        index = lax.broadcasted_iota(jnp.int32, (step, 2 * tok), 0) + at
        hot = jnp.where(index == ids, 1.0, 0.0).astype(BF16)
        return acc + dot(halves, hot)

    found = lax.fori_loop(
        0, place_ref.shape[1] // step, place_step, jnp.zeros((8, 2 * tok), F32)
    )
    pos = (found[0:1, :] * 64.0 + found[1:2, :]).astype(jnp.int32)
    posall[me_emb] = jnp.broadcast_to(pos, (8, 2 * tok))
    gall[me_emb] = grads_ref[...]
    table16[...] = table_ref[...].astype(BF16)
    pl.semaphore_wait(barrier, n_emb - 1 + n_chip - 1 + 1)

    pending = []
    first = []
    for k, peer in enumerate(emb_peers):
        one = copy(
            posall.at[me_emb], posall.at[me_emb], e_send.at[0, k], e_recv.at[0, k], me_dp, peer
        )
        one.start()
        first.append(one)
    second = []
    for k, peer in enumerate(emb_peers):
        one = copy(grads_ref, gall.at[me_emb], e_send.at[1, k], e_recv.at[1, k], me_dp, peer)
        one.start()
        second.append(one)
    pending += first + second
    for one in first:
        one.wait_recv()

    base = me_emb * rows
    kt = 256

    def lookup_step(e, carry):
        line = jnp.broadcast_to(posall[e][0:1, 0:tok] - base, (128, tok)).T
        line = jnp.concatenate([line] * (kt // 128), axis=1)
        acc = jnp.zeros((tok, 128), F32)
        for i in range(rows // kt):
            index = lax.broadcasted_iota(jnp.int32, (tok, kt), 1) + i * kt
            hot = jnp.where(index == line, 1.0, 0.0).astype(BF16)
            acc = acc + dot(hot, table16[i * kt : (i + 1) * kt, :])
        contrib[pl.ds(pl.multiple_of(e * tok, tok), tok), :] = acc.astype(BF16)
        return carry

    lax.fori_loop(0, n_emb, lookup_step, 0)
    third = []
    for k, peer in enumerate(emb_peers):
        one = copy(contrib, lbuf.at[k], e_send.at[2, k], e_recv.at[2, k], me_dp, peer)
        one.start()
        third.append(one)
    pending += third

    for one in second:
        one.wait_recv()
    half_rows = rows // 2
    pt = 128 if half_rows % 128 == 0 else half_rows

    def grad_step(i, carry):
        at = pl.multiple_of(i * pt, pt)
        index = lax.broadcasted_iota(jnp.int32, (pt, tok), 0) + (at + base)
        acc = jnp.zeros((pt, 128), F32)
        for e in range(n_emb):
            hot = jnp.where(index == posall[e][0:1, tok : 2 * tok], 1.0, 0.0).astype(BF16)
            acc = acc + dot(hot, gall[e])
        tpart[pl.ds(at, pt), :] = acc
        return carry

    lax.fori_loop(0, rows // pt, grad_step, 0)
    t_first = copy(
        tpart.at[pl.ds(pl.multiple_of(other * half_rows, 8), half_rows)],
        tpair,
        t_send.at[0, 0],
        t_recv.at[0, 0],
        partner,
        me_emb,
    )
    t_first.start()
    pending.append(t_first)

    for one in third:
        one.wait_recv()
    looked = contrib[...].astype(F32)
    for k in range(n_emb - 1):
        looked = looked + lbuf[k].astype(F32)
    values[...] = looked
    inverse_rms = lax.rsqrt(jnp.mean(looked * looked, axis=1, keepdims=True) + norm_eps)
    norm16 = (looked * inverse_rms * gain_ref[...]).astype(BF16)
    normed[...] = norm16
    normed_t[...] = norm16.astype(F32).T

    logit[...] = jnp.zeros_like(logit)

    def tower_step(j, carry):
        cols = pl.ds(pl.multiple_of(j * ht, ht), ht)
        gate = dot(normed[...], wg_ref[:, cols])
        up = dot(normed[...], wu_ref[:, cols])
        sig = jax.nn.sigmoid(gate)
        activated = gate * sig
        act[0, :, cols] = (up * (sig + activated * (1.0 - sig))).astype(BF16)
        act[1, :, cols] = activated.astype(BF16)
        hidden = (activated * up).astype(BF16)
        head = jnp.broadcast_to(wo_ref[:, cols].astype(F32), (8, ht)).astype(BF16)
        logit[...] += dot_nt(head, hidden)
        return carry

    lax.fori_loop(0, hid // ht, tower_step, 0)
    fourth = []
    for k, peer in enumerate(emb_peers):
        one = copy(logit, logit_in.at[k], e_send.at[3, k], e_recv.at[3, k], me_dp, peer)
        one.start()
        fourth.append(one)
    pending += fourth

    t_first.wait_recv()
    tsum[...] = tpart[pl.ds(pl.multiple_of(par * half_rows, 8), half_rows), :] + tpair[...]
    t_scatter = []
    for k, peer in enumerate(chip_peers):
        there = pl.multiple_of(lax.rem(chip + k + 1, n_chip) * t_rows, 8)
        one = copy(
            tsum.at[pl.ds(there, t_rows)],
            tin.at[k],
            t_send.at[1, k],
            t_recv.at[1, k],
            peer,
            me_emb,
        )
        one.start()
        t_scatter.append(one)
    pending += t_scatter

    bn[...] = jnp.zeros_like(bn)

    def back_step(j, carry):
        cols = pl.ds(pl.multiple_of(j * ht, ht), ht)
        head = wo_ref[:, cols].astype(F32)
        wg = (wg_ref[:, cols].astype(F32) * head).astype(BF16)
        wu = (wu_ref[:, cols].astype(F32) * head).astype(BF16)
        bn[...] += dot_nt(act[0, :, cols], wg) + dot_nt(act[1, :, cols], wu)
        return carry

    lax.fori_loop(0, hid // ht, back_step, 0)
    fifth = []
    for k, peer in enumerate(emb_peers):
        one = copy(
            bn.at[pl.ds(pl.multiple_of(peer * tok, tok), tok)],
            bn_in.at[k],
            e_send.at[4, k],
            e_recv.at[4, k],
            me_dp,
            peer,
        )
        one.start()
        fifth.append(one)
    pending += fifth

    for one in fourth:
        one.wait_recv()
    logits = logit[...]
    for k in range(n_emb - 1):
        logits = logits + logit_in[k]
    slope = loss_weight * (jax.nn.sigmoid(logits) - labels_ref[...])
    slopes[...] = slope
    lead = (normed_t[...] * slope[0:1, :]).astype(BF16)

    def weight_grads(which):
        for j in range(hid // ht):
            cols = slice(j * ht, (j + 1) * ht)
            head = wo_ref[:, cols].astype(F32) * scale
            part = (dot(lead, act[which, :, cols]) * head).astype(BF16)
            for b in range(ht // 128):
                at = j * ht + b * 128
                gpart[which, at : at + 128, :] = part[:, b * 128 : (b + 1) * 128]

    weight_grads(other)
    g_first = copy(gpart.at[other], gpair, g_send.at[0, 0], g_recv.at[0, 0], partner, me_emb)
    g_first.start()
    pending.append(g_first)
    weight_grads(par)

    for one in t_scatter:
        one.wait_recv()
    piece = tsum[pl.ds(pl.multiple_of(chip * t_rows, 8), t_rows), :]
    for k in range(n_chip - 1):
        piece = piece + tin[k]
    mine = pl.ds(pl.multiple_of(par * half_rows + chip * t_rows, 8), t_rows)
    tall[mine, :] = piece
    t_spread = []
    for k, peer in enumerate(chip_peers):
        one = copy(
            tall.at[mine], tall.at[mine], t_send.at[2, k], t_recv.at[2, k], peer, me_emb
        )
        one.start()
        t_spread.append(one)
    t_last = [
        copy(
            tall.at[mine],
            tall.at[mine],
            t_send.at[3, n_chip - 1],
            t_recv.at[3, n_chip - 1],
            partner,
            me_emb,
        )
    ]
    t_last[0].start()

    g_first.wait_recv()
    gsum[...] = (gpart[par].astype(F32) + gpair[...].astype(F32)).astype(BF16)
    g_scatter = []
    for k, peer in enumerate(chip_peers):
        there = pl.multiple_of(lax.rem(chip + k + 1, n_chip) * g_rows, 16)
        one = copy(
            gsum.at[pl.ds(there, g_rows)],
            gin.at[k],
            g_send.at[1, k],
            g_recv.at[1, k],
            peer,
            me_emb,
        )
        one.start()
        g_scatter.append(one)
    pending += g_scatter

    for one in fifth:
        one.wait_recv()
    own = pl.ds(pl.multiple_of(me_emb * tok, tok), tok)
    back = bn[own, :]
    for k in range(n_emb - 1):
        back = back + bn_in[k]
    slope_col = jnp.broadcast_to(slopes[0:1, own], (128, tok)).T
    scaled = back * slope_col * gain_ref[...]
    x = values[own, :]
    inv = lax.rsqrt(jnp.mean(x * x, axis=1, keepdims=True) + norm_eps)
    emb_ref[...] = inv * scaled - x * (inv * inv * inv) * jnp.mean(
        x * scaled, axis=1, keepdims=True
    )

    for k in range(n_chip - 1):
        t_spread[k].wait_recv()
        came = pl.ds(
            pl.multiple_of(par * half_rows + from_chip[k] * t_rows, 8), t_rows
        )
        one = copy(
            tall.at[came], tall.at[came], t_send.at[3, k], t_recv.at[3, k], partner, me_emb
        )
        one.start()
        t_last.append(one)
    pending += t_spread + t_last

    for one in g_scatter:
        one.wait_recv()
    piece = gsum[pl.ds(pl.multiple_of(chip * g_rows, 16), g_rows), :].astype(F32)
    for k in range(n_chip - 1):
        piece = piece + gin[k].astype(F32)
    mine = pl.ds(pl.multiple_of(chip * g_rows, 16), g_rows)
    gall_sum[par, mine, :] = piece.astype(BF16)
    g_spread = []
    for k, peer in enumerate(chip_peers):
        one = copy(
            gall_sum.at[par, mine],
            gall_sum.at[par, mine],
            g_send.at[2, k],
            g_recv.at[2, k],
            peer,
            me_emb,
        )
        one.start()
        g_spread.append(one)
    g_last = [
        copy(
            gall_sum.at[par, mine],
            gall_sum.at[par, mine],
            g_send.at[3, n_chip - 1],
            g_recv.at[3, n_chip - 1],
            partner,
            me_emb,
        )
    ]
    g_last[0].start()
    for one in t_last:
        one.wait_recv()
    total_ref[...] = tall[...]
    for k in range(n_chip - 1):
        g_spread[k].wait_recv()
        came = pl.ds(pl.multiple_of(from_chip[k] * g_rows, 16), g_rows)
        one = copy(
            gall_sum.at[par, came],
            gall_sum.at[par, came],
            g_send.at[3, k],
            g_recv.at[3, k],
            partner,
            me_emb,
        )
        one.start()
        g_last.append(one)
    pending += g_spread + g_last
    for one in g_last:
        one.wait_recv()
    for b in range(hid // 128):
        cols = slice(b * 128, (b + 1) * 128)
        gate_ref[:, cols] = gall_sum[0, cols, :]
        up_ref[:, cols] = gall_sum[1, cols, :]
    for one in pending:
        one.wait_send()


def on_device(
    cur_ids, prev_ids, prev_grads, row_place, table, accum, labels, gain, w_gate, w_up, w_out
):
    n_emb = lax.axis_size("emb")
    n_dp = lax.axis_size("dp")
    n_chip = n_dp // 2
    rows, width = table.shape
    tok = cur_ids.shape[0]
    group = tok * n_emb
    hid = w_gate.shape[1]
    scale = 1.0 / math.sqrt(tok * n_emb * n_dp)
    vmem = pl.BlockSpec(memory_space=pltpu.VMEM)
    n_peer = max(n_emb - 1, 1)
    dma = pltpu.SemaphoreType.DMA
    total, gate, up, emb_grad = pl.pallas_call(
        functools.partial(tower_kernel, n_dp, n_emb, scale),
        out_shape=(
            jax.ShapeDtypeStruct((rows, width), F32),
            jax.ShapeDtypeStruct((width, hid), BF16),
            jax.ShapeDtypeStruct((width, hid), BF16),
            jax.ShapeDtypeStruct((tok, width), F32),
        ),
        in_specs=[vmem] * 10,
        out_specs=(vmem,) * 4,
        scratch_shapes=[
            pltpu.VMEM((rows, width), BF16),
            pltpu.VMEM((n_emb, 8, 2 * tok), jnp.int32),
            pltpu.VMEM((n_emb, tok, width), BF16),
            pltpu.VMEM((group, width), BF16),
            pltpu.VMEM((n_peer, group, width), BF16),
            pltpu.VMEM((group, width), F32),
            pltpu.VMEM((group, width), BF16),
            pltpu.VMEM((width, group), F32),
            pltpu.VMEM((2, group, hid), BF16),
            pltpu.VMEM((8, group), F32),
            pltpu.VMEM((n_peer, 8, group), F32),
            pltpu.VMEM((8, group), F32),
            pltpu.VMEM((group, width), F32),
            pltpu.VMEM((n_peer, tok, width), F32),
            pltpu.VMEM((rows, width), F32),
            pltpu.VMEM((rows // 2, width), F32),
            pltpu.VMEM((rows // 2, width), F32),
            pltpu.VMEM((n_chip - 1, rows // n_dp, width), F32),
            pltpu.VMEM((rows, width), F32),
            pltpu.VMEM((2, hid, width), BF16),
            pltpu.VMEM((hid, width), BF16),
            pltpu.VMEM((hid, width), BF16),
            pltpu.VMEM((n_chip - 1, hid // n_chip, width), BF16),
            pltpu.VMEM((2, hid, width), BF16),
            dma((5, n_peer)),
            dma((5, n_peer)),
            dma((4, n_chip)),
            dma((4, n_chip)),
            dma((4, n_chip)),
            dma((4, n_chip)),
        ],
        compiler_params=pltpu.CompilerParams(
            collective_id=0, has_side_effects=True, vmem_limit_bytes=60 * 1024 * 1024
        ),
    )(
        cur_ids.reshape(1, -1),
        prev_ids.reshape(1, -1),
        prev_grads,
        row_place.reshape(1, -1),
        table,
        labels.reshape(1, -1),
        gain.reshape(1, -1),
        w_gate,
        w_up,
        w_out.reshape(1, -1),
    )
    new_accum = accum + total * total
    new_table = table - learn_rate * total * lax.rsqrt(new_accum)
    return (new_table, new_accum, gate.astype(F32), up.astype(F32), emb_grad)


def solution(mesh):
    placed = (
        P(("dp", "emb")),
        P(("dp", "emb")),
        P(("dp", "emb"), None),
        P(),
        P("emb", None),
        P("emb", None),
        P("dp"),
        P(),
        P(None, "emb"),
        P(None, "emb"),
        P("emb"),
    )
    return jax.shard_map(
        on_device,
        mesh=mesh,
        in_specs=placed,
        out_specs=(
            P("emb", None),
            P("emb", None),
            P(None, "emb"),
            P(None, "emb"),
            P(("dp", "emb"), None),
        ),
        check_vma=False,
    )
```

```python
import functools
import math

import jax
import jax.numpy as jnp
from jax import lax
from jax.experimental import pallas as pl
from jax.experimental.pallas import tpu as pltpu
from jax.sharding import PartitionSpec as P

loss_weight = 64.0
learn_rate = 0.1
norm_eps = 1e-06
MESH = pl.DeviceIdType.MESH
F32 = jnp.float32
BF16 = jnp.bfloat16


def dot(a, b):
    return jnp.dot(a, b, preferred_element_type=F32)


def dot_nt(a, b):
    return lax.dot_general(a, b, (((1,), (1,)), ((), ())), preferred_element_type=F32)


def tower_kernel(
    n_dp,
    n_emb,
    scale,
    cur_ref,
    prev_ref,
    grads_ref,
    place_ref,
    table_ref,
    labels_ref,
    gain_ref,
    wg_ref,
    wu_ref,
    wo_ref,
    total_ref,
    gate_ref,
    up_ref,
    emb_ref,
    table16,
    posall,
    gall,
    contrib,
    lbuf,
    values,
    normed,
    normed_t,
    act,
    logit,
    logit_in,
    slopes,
    bn,
    bn_in,
    tpart,
    tpair,
    tsum,
    tx_in,
    tz_out,
    tz_in,
    tall,
    gpart,
    gpair,
    gsum,
    gx_in,
    gz_out,
    gz_in,
    gtotal,
    e_send,
    e_recv,
    t_send,
    t_recv,
    g_send,
    g_recv,
):
    me_dp = lax.axis_index("dp")
    me_emb = lax.axis_index("emb")
    n_chip = n_dp // 2
    n_hi = n_chip // 2
    chip = me_dp // 2
    low = chip % 2
    high = chip // 2
    par = me_dp % 2
    other = 1 - par
    partner = me_dp + 1 - 2 * par
    beside = me_dp + 2 - 4 * low
    tok = grads_ref.shape[0]
    rows = table_ref.shape[0]
    hid = wg_ref.shape[1]
    ht = 256

    def copy(src, dst, send, recv, dp, emb):
        return pltpu.make_async_remote_copy(
            src_ref=src,
            dst_ref=dst,
            send_sem=send,
            recv_sem=recv,
            device_id=(dp, emb),
            device_id_type=MESH,
        )

    emb_peers = [lax.rem(me_emb + k, n_emb) for k in range(1, n_emb)]
    ahead = [lax.rem(high + k, n_hi) for k in range(n_hi)]
    behind = [lax.rem(high + n_hi - k, n_hi) for k in range(n_hi)]
    far_peers = [(2 * h + low) * 2 + par for h in ahead]
    pending = []

    class Reduce:

        def __init__(self, part, pair, acc, x_in, z_out, z_in, full, send, recv, align):
            self.part, self.pair, self.acc, self.x_in = part, pair, acc, x_in
            self.z_out, self.z_in, self.full = z_out, z_in, full
            self.send, self.recv, self.align = send, recv, align
            self.half = pair.shape[0]
            self.size = self.half // n_chip

        def rows(self, at, size):
            return pl.ds(pl.multiple_of(at, self.align), size)

        def piece(self, lo, hi):
            return self.rows((lo * n_hi + hi) * self.size, self.size)

        def place(self, lo, hi):
            return self.rows(par * self.half + (lo * n_hi + hi) * self.size, self.size)

        def go(self, src, dst, stage, k, dp):
            one = copy(src, dst, self.send.at[stage, k], self.recv.at[stage, k], dp, me_emb)
            one.start()
            pending.append(one)
            return one

        def start(self):
            away = self.rows(other * self.half, self.half)
            self.first = self.go(self.part.at[away], self.pair, 0, 0, partner)

        def stage_x(self):
            self.first.wait_recv()
            kept = self.part[self.rows(par * self.half, self.half), :]
            joined = kept.astype(F32) + self.pair[...].astype(F32)
            self.acc[...] = joined.astype(self.acc.dtype)
            self.x = {}
            for k in list(range(1, n_hi)) + [0]:
                self.x[k] = self.go(
                    self.acc.at[self.piece(1 - low, ahead[k])], self.x_in.at[k], 1, k, beside
                )

        def joined(self, k):
            self.x[k].wait_recv()
            kept = self.acc[self.piece(low, ahead[k]), :].astype(F32)
            return kept + self.x_in[k].astype(F32)

        def stage_z(self):
            self.z = []
            for k in range(1, n_hi):
                self.z_out[k - 1] = self.joined(k).astype(self.z_out.dtype)
                self.z.append(
                    self.go(self.z_out.at[k - 1], self.z_in.at[k - 1], 2, k, far_peers[k])
                )

        def stage_sum(self):
            total = self.joined(0)
            for k, one in enumerate(self.z):
                one.wait_recv()
                total = total + self.z_in[k].astype(F32)
            mine = self.place(low, high)
            self.full[mine, :] = total.astype(self.full.dtype)
            view = self.full.at[mine]
            self.far = [self.go(view, view, 3, k, far_peers[k]) for k in range(1, n_hi)]
            self.near = [self.go(view, view, 4, 0, beside)]
            self.last = [self.go(view, view, 5, 0, partner)]

        def spread_z(self):
            for k in range(1, n_hi):
                self.far[k - 1].wait_recv()
                view = self.full.at[self.place(low, behind[k])]
                self.near.append(self.go(view, view, 4, k, beside))
                self.last.append(self.go(view, view, 5, k, partner))

        def spread_x(self):
            for k in range(n_hi):
                self.near[k].wait_recv()
                view = self.full.at[self.place(1 - low, behind[k])]
                self.last.append(self.go(view, view, 5, n_hi + k, partner))

        def finish(self):
            for one in self.last:
                one.wait_recv()

    sums = Reduce(tpart, tpair, tsum, tx_in, tz_out, tz_in, tall, t_send, t_recv, 8)
    tower = Reduce(gpart, gpair, gsum, gx_in, gz_out, gz_in, gtotal, g_send, g_recv, 16)

    barrier = pltpu.get_barrier_semaphore()
    for peer in emb_peers:
        pl.semaphore_signal(barrier, inc=1, device_id=(me_dp, peer), device_id_type=MESH)
    for peer in far_peers[1:] + [beside]:
        pl.semaphore_signal(barrier, inc=1, device_id=(peer, me_emb), device_id_type=MESH)
    pl.semaphore_signal(barrier, inc=1, device_id=(partner, me_emb), device_id_type=MESH)

    ids = jnp.concatenate([cur_ref[...], prev_ref[...]], axis=1)
    step = 512

    def place_step(i, acc):
        at = pl.multiple_of(i * step, step)
        part = place_ref[:, pl.ds(at, step)]
        both = jnp.broadcast_to(part, (8, step))
        lane_row = lax.broadcasted_iota(jnp.int32, (8, step), 0)
        halves = jnp.where(lane_row == 0, both >> 6, both & 63).astype(F32).astype(BF16)
        index = lax.broadcasted_iota(jnp.int32, (step, 2 * tok), 0) + at
        hot = jnp.where(index == ids, 1.0, 0.0).astype(BF16)
        return acc + dot(halves, hot)

    found = lax.fori_loop(
        0, place_ref.shape[1] // step, place_step, jnp.zeros((8, 2 * tok), F32)
    )
    pos = (found[0:1, :] * 64.0 + found[1:2, :]).astype(jnp.int32)
    posall[me_emb] = jnp.broadcast_to(pos, (8, 2 * tok))
    gall[me_emb] = grads_ref[...]
    table16[...] = table_ref[...].astype(BF16)
    pl.semaphore_wait(barrier, n_emb - 1 + n_hi - 1 + 2)

    first = []
    for k, peer in enumerate(emb_peers):
        one = copy(
            posall.at[me_emb], posall.at[me_emb], e_send.at[0, k], e_recv.at[0, k], me_dp, peer
        )
        one.start()
        first.append(one)
    second = []
    for k, peer in enumerate(emb_peers):
        one = copy(grads_ref, gall.at[me_emb], e_send.at[1, k], e_recv.at[1, k], me_dp, peer)
        one.start()
        second.append(one)
    pending += first + second
    for one in first:
        one.wait_recv()

    base = me_emb * rows
    kt = 256

    def lookup_step(e, carry):
        line = jnp.broadcast_to(posall[e][0:1, 0:tok] - base, (128, tok)).T
        line = jnp.concatenate([line] * (kt // 128), axis=1)
        acc = jnp.zeros((tok, 128), F32)
        for i in range(rows // kt):
            index = lax.broadcasted_iota(jnp.int32, (tok, kt), 1) + i * kt
            hot = jnp.where(index == line, 1.0, 0.0).astype(BF16)
            acc = acc + dot(hot, table16[i * kt : (i + 1) * kt, :])
        contrib[pl.ds(pl.multiple_of(e * tok, tok), tok), :] = acc.astype(BF16)
        return carry

    lax.fori_loop(0, n_emb, lookup_step, 0)
    third = []
    for k, peer in enumerate(emb_peers):
        one = copy(contrib, lbuf.at[k], e_send.at[2, k], e_recv.at[2, k], me_dp, peer)
        one.start()
        third.append(one)
    pending += third

    for one in second:
        one.wait_recv()
    half_rows = rows // 2
    pt = 128 if half_rows % 128 == 0 else half_rows

    def grad_step(i, carry):
        at = pl.multiple_of(i * pt, pt)
        index = lax.broadcasted_iota(jnp.int32, (pt, tok), 0) + (at + base)
        acc = jnp.zeros((pt, 128), F32)
        for e in range(n_emb):
            hot = jnp.where(index == posall[e][0:1, tok : 2 * tok], 1.0, 0.0).astype(BF16)
            acc = acc + dot(hot, gall[e])
        tpart[pl.ds(at, pt), :] = acc
        return carry

    lax.fori_loop(0, rows // pt, grad_step, 0)
    sums.start()
    sums.stage_x()

    for one in third:
        one.wait_recv()
    looked = contrib[...].astype(F32)
    for k in range(n_emb - 1):
        looked = looked + lbuf[k].astype(F32)
    values[...] = looked
    inverse_rms = lax.rsqrt(jnp.mean(looked * looked, axis=1, keepdims=True) + norm_eps)
    norm16 = (looked * inverse_rms * gain_ref[...]).astype(BF16)
    normed[...] = norm16
    normed_t[...] = norm16.astype(F32).T

    logit[...] = jnp.zeros_like(logit)

    def tower_step(j, carry):
        cols = pl.ds(pl.multiple_of(j * ht, ht), ht)
        gate = dot(normed[...], wg_ref[:, cols])
        up = dot(normed[...], wu_ref[:, cols])
        sig = jax.nn.sigmoid(gate)
        activated = gate * sig
        act[0, :, cols] = (up * (sig + activated * (1.0 - sig))).astype(BF16)
        act[1, :, cols] = activated.astype(BF16)
        hidden = (activated * up).astype(BF16)
        head = jnp.broadcast_to(wo_ref[:, cols].astype(F32), (8, ht)).astype(BF16)
        logit[...] += dot_nt(head, hidden)
        return carry

    tiles = hid // ht
    some = max(1, 5 * tiles // 8)
    lax.fori_loop(0, some, tower_step, 0)
    sums.stage_z()
    lax.fori_loop(some, tiles, tower_step, 0)
    fourth = []
    for k, peer in enumerate(emb_peers):
        one = copy(logit, logit_in.at[k], e_send.at[3, k], e_recv.at[3, k], me_dp, peer)
        one.start()
        fourth.append(one)
    pending += fourth

    bn[...] = jnp.zeros_like(bn)

    def back_step(j, carry):
        cols = pl.ds(pl.multiple_of(j * ht, ht), ht)
        head = wo_ref[:, cols].astype(F32)
        wg = (wg_ref[:, cols].astype(F32) * head).astype(BF16)
        wu = (wu_ref[:, cols].astype(F32) * head).astype(BF16)
        bn[...] += dot_nt(act[0, :, cols], wg) + dot_nt(act[1, :, cols], wu)
        return carry

    lax.fori_loop(0, hid // ht, back_step, 0)
    fifth = []
    for k, peer in enumerate(emb_peers):
        one = copy(
            bn.at[pl.ds(pl.multiple_of(peer * tok, tok), tok)],
            bn_in.at[k],
            e_send.at[4, k],
            e_recv.at[4, k],
            me_dp,
            peer,
        )
        one.start()
        fifth.append(one)
    pending += fifth

    for one in fourth:
        one.wait_recv()
    logits = logit[...]
    for k in range(n_emb - 1):
        logits = logits + logit_in[k]
    slope = loss_weight * (jax.nn.sigmoid(logits) - labels_ref[...])
    slopes[...] = slope
    lead = (normed_t[...] * slope[0:1, :]).astype(BF16)

    def weight_grads(which):
        for j in range(hid // ht):
            cols = slice(j * ht, (j + 1) * ht)
            head = wo_ref[:, cols].astype(F32) * scale
            part = (dot(lead, act[which, :, cols]) * head).astype(BF16)
            for b in range(ht // 128):
                at = j * ht + b * 128
                gpart[pl.ds(pl.multiple_of(which * hid + at, 128), 128), :] = part[:, b * 128 : (b + 1) * 128]

    weight_grads(other)
    tower.start()
    sums.stage_sum()
    weight_grads(par)
    tower.stage_x()

    for one in fifth:
        one.wait_recv()
    own = pl.ds(pl.multiple_of(me_emb * tok, tok), tok)
    back = bn[own, :]
    for k in range(n_emb - 1):
        back = back + bn_in[k]
    slope_col = jnp.broadcast_to(slopes[0:1, own], (128, tok)).T
    scaled = back * slope_col * gain_ref[...]
    x = values[own, :]
    inv = lax.rsqrt(jnp.mean(x * x, axis=1, keepdims=True) + norm_eps)
    emb_ref[...] = inv * scaled - x * (inv * inv * inv) * jnp.mean(
        x * scaled, axis=1, keepdims=True
    )

    tower.stage_z()
    sums.spread_z()
    tower.stage_sum()
    sums.spread_x()
    tower.spread_z()
    tower.spread_x()
    sums.finish()
    total_ref[...] = tall[...]
    tower.finish()
    for b in range(hid // 128):
        cols = slice(b * 128, (b + 1) * 128)
        gate_ref[:, cols] = gtotal[cols, :]
        up_ref[:, cols] = gtotal[hid + b * 128 : hid + (b + 1) * 128, :]
    for one in pending:
        one.wait_send()


def on_device(
    cur_ids, prev_ids, prev_grads, row_place, table, accum, labels, gain, w_gate, w_up, w_out
):
    n_emb = lax.axis_size("emb")
    n_dp = lax.axis_size("dp")
    n_chip = n_dp // 2
    n_hi = n_chip // 2
    rows, width = table.shape
    tok = cur_ids.shape[0]
    group = tok * n_emb
    hid = w_gate.shape[1]
    scale = 1.0 / math.sqrt(tok * n_emb * n_dp)
    vmem = pl.BlockSpec(memory_space=pltpu.VMEM)
    n_peer = max(n_emb - 1, 1)
    dma = pltpu.SemaphoreType.DMA
    total, gate, up, emb_grad = pl.pallas_call(
        functools.partial(tower_kernel, n_dp, n_emb, scale),
        out_shape=(
            jax.ShapeDtypeStruct((rows, width), F32),
            jax.ShapeDtypeStruct((width, hid), BF16),
            jax.ShapeDtypeStruct((width, hid), BF16),
            jax.ShapeDtypeStruct((tok, width), F32),
        ),
        in_specs=[vmem] * 10,
        out_specs=(vmem,) * 4,
        scratch_shapes=[
            pltpu.VMEM((rows, width), BF16),
            pltpu.VMEM((n_emb, 8, 2 * tok), jnp.int32),
            pltpu.VMEM((n_emb, tok, width), BF16),
            pltpu.VMEM((group, width), BF16),
            pltpu.VMEM((n_peer, group, width), BF16),
            pltpu.VMEM((group, width), F32),
            pltpu.VMEM((group, width), BF16),
            pltpu.VMEM((width, group), F32),
            pltpu.VMEM((2, group, hid), BF16),
            pltpu.VMEM((8, group), F32),
            pltpu.VMEM((n_peer, 8, group), F32),
            pltpu.VMEM((8, group), F32),
            pltpu.VMEM((group, width), F32),
            pltpu.VMEM((n_peer, tok, width), F32),
            pltpu.VMEM((rows, width), F32),
            pltpu.VMEM((rows // 2, width), F32),
            pltpu.VMEM((rows // 2, width), F32),
            pltpu.VMEM((n_hi, rows // n_dp, width), F32),
            pltpu.VMEM((n_hi - 1, rows // n_dp, width), F32),
            pltpu.VMEM((n_hi - 1, rows // n_dp, width), F32),
            pltpu.VMEM((rows, width), F32),
            pltpu.VMEM((2 * hid, width), BF16),
            pltpu.VMEM((hid, width), BF16),
            pltpu.VMEM((hid, width), BF16),
            pltpu.VMEM((n_hi, hid // n_chip, width), BF16),
            pltpu.VMEM((n_hi - 1, hid // n_chip, width), BF16),
            pltpu.VMEM((n_hi - 1, hid // n_chip, width), BF16),
            pltpu.VMEM((2 * hid, width), BF16),
            dma((5, n_peer)),
            dma((5, n_peer)),
            dma((6, 2 * n_hi)),
            dma((6, 2 * n_hi)),
            dma((6, 2 * n_hi)),
            dma((6, 2 * n_hi)),
        ],
        compiler_params=pltpu.CompilerParams(
            collective_id=0, has_side_effects=True, vmem_limit_bytes=60 * 1024 * 1024
        ),
    )(
        cur_ids.reshape(1, -1),
        prev_ids.reshape(1, -1),
        prev_grads,
        row_place.reshape(1, -1),
        table,
        labels.reshape(1, -1),
        gain.reshape(1, -1),
        w_gate,
        w_up,
        w_out.reshape(1, -1),
    )
    new_accum = accum + total * total
    new_table = table - learn_rate * total * lax.rsqrt(new_accum)
    return (new_table, new_accum, gate.astype(F32), up.astype(F32), emb_grad)


def solution(mesh):
    placed = (
        P(("dp", "emb")),
        P(("dp", "emb")),
        P(("dp", "emb"), None),
        P(),
        P("emb", None),
        P("emb", None),
        P("dp"),
        P(),
        P(None, "emb"),
        P(None, "emb"),
        P("emb"),
    )
    return jax.shard_map(
        on_device,
        mesh=mesh,
        in_specs=placed,
        out_specs=(
            P("emb", None),
            P("emb", None),
            P(None, "emb"),
            P(None, "emb"),
            P(("dp", "emb"), None),
        ),
        check_vma=False,
    )
```

```python
import functools
import math

import jax
import jax.numpy as jnp
from jax import lax
from jax.experimental import pallas as pl
from jax.experimental.pallas import tpu as pltpu
from jax.sharding import PartitionSpec as P

loss_weight = 64.0
learn_rate = 0.1
norm_eps = 1e-06
MESH = pl.DeviceIdType.MESH
F32 = jnp.float32
BF16 = jnp.bfloat16


def dot(a, b):
    return jnp.dot(a, b, preferred_element_type=F32)


def dot_nt(a, b):
    return lax.dot_general(a, b, (((1,), (1,)), ((), ())), preferred_element_type=F32)


def tower_kernel(
    n_dp,
    n_emb,
    scale,
    cur_ref,
    prev_ref,
    grads_ref,
    place_ref,
    table_ref,
    accum_ref,
    labels_ref,
    gain_ref,
    wg_ref,
    wu_ref,
    wo_ref,
    new_table_ref,
    new_accum_ref,
    gate_ref,
    up_ref,
    emb_ref,
    table16,
    posall,
    gall,
    contrib,
    lbuf,
    values,
    normed,
    normed_t,
    act,
    logit,
    logit_in,
    slopes,
    bn,
    bn_in,
    tpart,
    tpair,
    tsum,
    tx_in,
    tz_out,
    tz_in,
    tall,
    gpart,
    gpair,
    gsum,
    gx_in,
    gz_out,
    gz_in,
    gtotal,
    e_send,
    e_recv,
    t_send,
    t_recv,
    g_send,
    g_recv,
):
    me_dp = lax.axis_index("dp")
    me_emb = lax.axis_index("emb")
    n_chip = n_dp // 2
    n_hi = n_chip // 2
    chip = me_dp // 2
    low = chip % 2
    high = chip // 2
    par = me_dp % 2
    other = 1 - par
    partner = me_dp + 1 - 2 * par
    beside = me_dp + 2 - 4 * low
    tok = grads_ref.shape[0]
    rows = table_ref.shape[0]
    hid = wg_ref.shape[1]
    ht = 256

    def copy(src, dst, send, recv, dp, emb):
        return pltpu.make_async_remote_copy(
            src_ref=src,
            dst_ref=dst,
            send_sem=send,
            recv_sem=recv,
            device_id=(dp, emb),
            device_id_type=MESH,
        )

    emb_peers = [lax.rem(me_emb + k, n_emb) for k in range(1, n_emb)]
    ahead = [lax.rem(high + k, n_hi) for k in range(n_hi)]
    behind = [lax.rem(high + n_hi - k, n_hi) for k in range(n_hi)]
    far_peers = [(2 * h + low) * 2 + par for h in ahead]
    pending = []

    class Reduce:

        def __init__(self, part, pair, acc, x_in, z_out, z_in, full, send, recv, align):
            self.part, self.pair, self.acc, self.x_in = part, pair, acc, x_in
            self.z_out, self.z_in, self.full = z_out, z_in, full
            self.send, self.recv, self.align = send, recv, align
            self.half = pair.shape[0]
            self.size = self.half // n_chip

        def rows(self, at, size):
            return pl.ds(pl.multiple_of(at, self.align), size)

        def piece(self, lo, hi):
            return self.rows((lo * n_hi + hi) * self.size, self.size)

        def place(self, lo, hi):
            return self.rows(par * self.half + (lo * n_hi + hi) * self.size, self.size)

        def go(self, src, dst, stage, k, dp):
            one = copy(src, dst, self.send.at[stage, k], self.recv.at[stage, k], dp, me_emb)
            one.start()
            pending.append(one)
            return one

        def start(self):
            away = self.rows(other * self.half, self.half)
            self.first = self.go(self.part.at[away], self.pair, 0, 0, partner)

        def stage_x(self):
            self.first.wait_recv()
            kept = self.part[self.rows(par * self.half, self.half), :]
            joined = kept.astype(F32) + self.pair[...].astype(F32)
            self.acc[...] = joined.astype(self.acc.dtype)
            self.x = {}
            for k in list(range(1, n_hi)) + [0]:
                self.x[k] = self.go(
                    self.acc.at[self.piece(1 - low, ahead[k])], self.x_in.at[k], 1, k, beside
                )

        def joined(self, k):
            self.x[k].wait_recv()
            kept = self.acc[self.piece(low, ahead[k]), :].astype(F32)
            return kept + self.x_in[k].astype(F32)

        def stage_z(self):
            self.z = []
            for k in range(1, n_hi):
                self.z_out[k - 1] = self.joined(k).astype(self.z_out.dtype)
                self.z.append(
                    self.go(self.z_out.at[k - 1], self.z_in.at[k - 1], 2, k, far_peers[k])
                )

        def stage_sum(self):
            total = self.joined(0)
            for k, one in enumerate(self.z):
                one.wait_recv()
                total = total + self.z_in[k].astype(F32)
            mine = self.place(low, high)
            self.full[mine, :] = total.astype(self.full.dtype)
            view = self.full.at[mine]
            self.far = [self.go(view, view, 3, k, far_peers[k]) for k in range(1, n_hi)]
            self.near = [self.go(view, view, 4, 0, beside)]
            self.last = [self.go(view, view, 5, 0, partner)]

        def spread_z(self):
            for k in range(1, n_hi):
                self.far[k - 1].wait_recv()
                view = self.full.at[self.place(low, behind[k])]
                self.near.append(self.go(view, view, 4, k, beside))
                self.last.append(self.go(view, view, 5, k, partner))

        def spread_x(self):
            for k in range(n_hi):
                self.near[k].wait_recv()
                view = self.full.at[self.place(1 - low, behind[k])]
                self.last.append(self.go(view, view, 5, n_hi + k, partner))

        def finish(self):
            for one in self.last:
                one.wait_recv()

    sums = Reduce(tpart, tpair, tsum, tx_in, tz_out, tz_in, tall, t_send, t_recv, 8)
    tower = Reduce(gpart, gpair, gsum, gx_in, gz_out, gz_in, gtotal, g_send, g_recv, 16)

    barrier = pltpu.get_barrier_semaphore()
    for peer in emb_peers:
        pl.semaphore_signal(barrier, inc=1, device_id=(me_dp, peer), device_id_type=MESH)
    for peer in far_peers[1:] + [beside]:
        pl.semaphore_signal(barrier, inc=1, device_id=(peer, me_emb), device_id_type=MESH)
    pl.semaphore_signal(barrier, inc=1, device_id=(partner, me_emb), device_id_type=MESH)

    ids = jnp.concatenate([cur_ref[...], prev_ref[...]], axis=1)
    step = 512

    def place_step(i, acc):
        at = pl.multiple_of(i * step, step)
        part = place_ref[:, pl.ds(at, step)]
        both = jnp.broadcast_to(part, (8, step))
        lane_row = lax.broadcasted_iota(jnp.int32, (8, step), 0)
        halves = jnp.where(lane_row == 0, both >> 6, both & 63).astype(F32).astype(BF16)
        index = lax.broadcasted_iota(jnp.int32, (step, 2 * tok), 0) + at
        hot = jnp.where(index == ids, 1.0, 0.0).astype(BF16)
        return acc + dot(halves, hot)

    found = lax.fori_loop(
        0, place_ref.shape[1] // step, place_step, jnp.zeros((8, 2 * tok), F32)
    )
    pos = (found[0:1, :] * 64.0 + found[1:2, :]).astype(jnp.int32)
    posall[me_emb] = jnp.broadcast_to(pos, (8, 2 * tok))
    gall[me_emb] = grads_ref[...]
    table16[...] = table_ref[...].astype(BF16)
    pl.semaphore_wait(barrier, n_emb - 1 + n_hi - 1 + 2)

    first = []
    for k, peer in enumerate(emb_peers):
        one = copy(
            posall.at[me_emb], posall.at[me_emb], e_send.at[0, k], e_recv.at[0, k], me_dp, peer
        )
        one.start()
        first.append(one)
    second = []
    for k, peer in enumerate(emb_peers):
        one = copy(grads_ref, gall.at[me_emb], e_send.at[1, k], e_recv.at[1, k], me_dp, peer)
        one.start()
        second.append(one)
    pending += first + second
    for one in first:
        one.wait_recv()

    base = me_emb * rows
    kt = 256

    def lookup_step(e, carry):
        line = jnp.broadcast_to(posall[e][0:1, 0:tok] - base, (128, tok)).T
        line = jnp.concatenate([line] * (kt // 128), axis=1)
        acc = jnp.zeros((tok, 128), F32)
        for i in range(rows // kt):
            index = lax.broadcasted_iota(jnp.int32, (tok, kt), 1) + i * kt
            hot = jnp.where(index == line, 1.0, 0.0).astype(BF16)
            acc = acc + dot(hot, table16[i * kt : (i + 1) * kt, :])
        contrib[pl.ds(pl.multiple_of(e * tok, tok), tok), :] = acc.astype(BF16)
        return carry

    lax.fori_loop(0, n_emb, lookup_step, 0)
    third = []
    for k, peer in enumerate(emb_peers):
        one = copy(contrib, lbuf.at[k], e_send.at[2, k], e_recv.at[2, k], me_dp, peer)
        one.start()
        third.append(one)
    pending += third

    for one in second:
        one.wait_recv()
    half_rows = rows // 2
    pt = 128 if half_rows % 128 == 0 else half_rows

    def grad_step(i, carry):
        at = pl.multiple_of(i * pt, pt)
        index = lax.broadcasted_iota(jnp.int32, (pt, tok), 0) + (at + base)
        acc = jnp.zeros((pt, 128), F32)
        for e in range(n_emb):
            hot = jnp.where(index == posall[e][0:1, tok : 2 * tok], 1.0, 0.0).astype(BF16)
            acc = acc + dot(hot, gall[e])
        tpart[pl.ds(at, pt), :] = acc
        return carry

    lax.fori_loop(0, rows // pt, grad_step, 0)
    sums.start()
    sums.stage_x()

    for one in third:
        one.wait_recv()
    looked = contrib[...].astype(F32)
    for k in range(n_emb - 1):
        looked = looked + lbuf[k].astype(F32)
    values[...] = looked
    inverse_rms = lax.rsqrt(jnp.mean(looked * looked, axis=1, keepdims=True) + norm_eps)
    norm16 = (looked * inverse_rms * gain_ref[...]).astype(BF16)
    normed[...] = norm16
    normed_t[...] = norm16.astype(F32).T

    logit[...] = jnp.zeros_like(logit)

    def tower_step(j, carry):
        cols = pl.ds(pl.multiple_of(j * ht, ht), ht)
        gate = dot(normed[...], wg_ref[:, cols])
        up = dot(normed[...], wu_ref[:, cols])
        sig = jax.nn.sigmoid(gate)
        activated = gate * sig
        act[0, :, cols] = (up * (sig + activated * (1.0 - sig))).astype(BF16)
        act[1, :, cols] = activated.astype(BF16)
        hidden = (activated * up).astype(BF16)
        head = jnp.broadcast_to(wo_ref[:, cols].astype(F32), (8, ht)).astype(BF16)
        logit[...] += dot_nt(head, hidden)
        return carry

    tiles = hid // ht
    some = max(1, 5 * tiles // 8)
    lax.fori_loop(0, some, tower_step, 0)
    sums.stage_z()
    lax.fori_loop(some, tiles, tower_step, 0)
    fourth = []
    for k, peer in enumerate(emb_peers):
        one = copy(logit, logit_in.at[k], e_send.at[3, k], e_recv.at[3, k], me_dp, peer)
        one.start()
        fourth.append(one)
    pending += fourth

    bn[...] = jnp.zeros_like(bn)

    def back_step(j, carry):
        cols = pl.ds(pl.multiple_of(j * ht, ht), ht)
        head = wo_ref[:, cols].astype(F32)
        wg = (wg_ref[:, cols].astype(F32) * head).astype(BF16)
        wu = (wu_ref[:, cols].astype(F32) * head).astype(BF16)
        bn[...] += dot_nt(act[0, :, cols], wg) + dot_nt(act[1, :, cols], wu)
        return carry

    lax.fori_loop(0, hid // ht, back_step, 0)
    fifth = []
    for k, peer in enumerate(emb_peers):
        one = copy(
            bn.at[pl.ds(pl.multiple_of(peer * tok, tok), tok)],
            bn_in.at[k],
            e_send.at[4, k],
            e_recv.at[4, k],
            me_dp,
            peer,
        )
        one.start()
        fifth.append(one)
    pending += fifth

    for one in fourth:
        one.wait_recv()
    logits = logit[...]
    for k in range(n_emb - 1):
        logits = logits + logit_in[k]
    slope = loss_weight * (jax.nn.sigmoid(logits) - labels_ref[...])
    slopes[...] = slope
    lead = (normed_t[...] * slope[0:1, :]).astype(BF16)

    def weight_grads(which):
        for j in range(hid // ht):
            cols = slice(j * ht, (j + 1) * ht)
            head = wo_ref[:, cols].astype(F32) * scale
            part = (dot(lead, act[which, :, cols]) * head).astype(BF16)
            for b in range(ht // 128):
                at = j * ht + b * 128
                gpart[pl.ds(pl.multiple_of(which * hid + at, 128), 128), :] = part[:, b * 128 : (b + 1) * 128]

    weight_grads(other)
    tower.start()
    sums.stage_sum()
    weight_grads(par)
    tower.stage_x()

    for one in fifth:
        one.wait_recv()
    own = pl.ds(pl.multiple_of(me_emb * tok, tok), tok)
    back = bn[own, :]
    for k in range(n_emb - 1):
        back = back + bn_in[k]
    slope_col = jnp.broadcast_to(slopes[0:1, own], (128, tok)).T
    scaled = back * slope_col * gain_ref[...]
    x = values[own, :]
    inv = lax.rsqrt(jnp.mean(x * x, axis=1, keepdims=True) + norm_eps)
    emb_ref[...] = inv * scaled - x * (inv * inv * inv) * jnp.mean(
        x * scaled, axis=1, keepdims=True
    )

    tower.stage_z()
    sums.spread_z()
    tower.stage_sum()
    sums.spread_x()
    tower.spread_z()
    tower.spread_x()
    sums.finish()
    summed = tall[...]
    squares = accum_ref[...] + summed * summed
    new_accum_ref[...] = squares
    new_table_ref[...] = table_ref[...] - learn_rate * summed * lax.rsqrt(squares)
    tower.finish()
    for b in range(hid // 128):
        cols = slice(b * 128, (b + 1) * 128)
        gate_ref[:, cols] = gtotal[cols, :].astype(F32)
        up_ref[:, cols] = gtotal[hid + b * 128 : hid + (b + 1) * 128, :].astype(F32)
    for one in pending:
        one.wait_send()


def on_device(
    cur_ids, prev_ids, prev_grads, row_place, table, accum, labels, gain, w_gate, w_up, w_out
):
    n_emb = lax.axis_size("emb")
    n_dp = lax.axis_size("dp")
    n_chip = n_dp // 2
    n_hi = n_chip // 2
    rows, width = table.shape
    tok = cur_ids.shape[0]
    group = tok * n_emb
    hid = w_gate.shape[1]
    scale = 1.0 / math.sqrt(tok * n_emb * n_dp)
    vmem = pl.BlockSpec(memory_space=pltpu.VMEM)
    n_peer = max(n_emb - 1, 1)
    dma = pltpu.SemaphoreType.DMA
    return pl.pallas_call(
        functools.partial(tower_kernel, n_dp, n_emb, scale),
        out_shape=(
            jax.ShapeDtypeStruct((rows, width), F32),
            jax.ShapeDtypeStruct((rows, width), F32),
            jax.ShapeDtypeStruct((width, hid), F32),
            jax.ShapeDtypeStruct((width, hid), F32),
            jax.ShapeDtypeStruct((tok, width), F32),
        ),
        in_specs=[vmem] * 11,
        out_specs=(vmem,) * 5,
        scratch_shapes=[
            pltpu.VMEM((rows, width), BF16),
            pltpu.VMEM((n_emb, 8, 2 * tok), jnp.int32),
            pltpu.VMEM((n_emb, tok, width), BF16),
            pltpu.VMEM((group, width), BF16),
            pltpu.VMEM((n_peer, group, width), BF16),
            pltpu.VMEM((group, width), F32),
            pltpu.VMEM((group, width), BF16),
            pltpu.VMEM((width, group), F32),
            pltpu.VMEM((2, group, hid), BF16),
            pltpu.VMEM((8, group), F32),
            pltpu.VMEM((n_peer, 8, group), F32),
            pltpu.VMEM((8, group), F32),
            pltpu.VMEM((group, width), F32),
            pltpu.VMEM((n_peer, tok, width), F32),
            pltpu.VMEM((rows, width), F32),
            pltpu.VMEM((rows // 2, width), F32),
            pltpu.VMEM((rows // 2, width), F32),
            pltpu.VMEM((n_hi, rows // n_dp, width), F32),
            pltpu.VMEM((n_hi - 1, rows // n_dp, width), F32),
            pltpu.VMEM((n_hi - 1, rows // n_dp, width), F32),
            pltpu.VMEM((rows, width), F32),
            pltpu.VMEM((2 * hid, width), BF16),
            pltpu.VMEM((hid, width), BF16),
            pltpu.VMEM((hid, width), BF16),
            pltpu.VMEM((n_hi, hid // n_chip, width), BF16),
            pltpu.VMEM((n_hi - 1, hid // n_chip, width), BF16),
            pltpu.VMEM((n_hi - 1, hid // n_chip, width), BF16),
            pltpu.VMEM((2 * hid, width), BF16),
            dma((5, n_peer)),
            dma((5, n_peer)),
            dma((6, 2 * n_hi)),
            dma((6, 2 * n_hi)),
            dma((6, 2 * n_hi)),
            dma((6, 2 * n_hi)),
        ],
        compiler_params=pltpu.CompilerParams(
            collective_id=0, has_side_effects=True, vmem_limit_bytes=60 * 1024 * 1024
        ),
    )(
        cur_ids.reshape(1, -1),
        prev_ids.reshape(1, -1),
        prev_grads,
        row_place.reshape(1, -1),
        table,
        accum,
        labels.reshape(1, -1),
        gain.reshape(1, -1),
        w_gate,
        w_up,
        w_out.reshape(1, -1),
    )


def solution(mesh):
    placed = (
        P(("dp", "emb")),
        P(("dp", "emb")),
        P(("dp", "emb"), None),
        P(),
        P("emb", None),
        P("emb", None),
        P("dp"),
        P(),
        P(None, "emb"),
        P(None, "emb"),
        P("emb"),
    )
    return jax.shard_map(
        on_device,
        mesh=mesh,
        in_specs=placed,
        out_specs=(
            P("emb", None),
            P("emb", None),
            P(None, "emb"),
            P(None, "emb"),
            P(("dp", "emb"), None),
        ),
        check_vma=False,
    )
```
